32 devices in a mesh: rep: 2 (over x), shard: 16 (over z, y, core).
Axes of the slice: x: 2, y: 2, z: 4, core: 2. Of those that a mesh axis runs over, the one named last changes fastest.
Arguments:
- features: float32 [16384, 256], P(('rep', 'shard')), may hold values from -6 to 6
- seed_self: float32 [4096, 256], P(('rep', 'shard')), may hold values from -6 to 6
- hub_ids: int32 [4096], P(('rep', 'shard')), may hold values from 0 to 511
- requests: int32 [512, 32], P(('rep', 'shard')), may hold values from 0 to 511
- counts: int32 [512], P(('rep', 'shard')), may hold values from 1 to 32, as said below
- neighbors: int32 [4096, 15], P(('rep', 'shard')), may hold values from 0 to 767
- weight: float32 [256, 256], replicated, may hold values from -1 to 1
- out_bias: float32 [256], replicated, may hold values from -4 to 4
Outputs:
- embedded: float32 [4096, 256], P(('rep', 'shard'))
The draws below stay inside these ranges and needn't reach their ends.
Inputs may be any that keep to these rules, and one draw needn't show every extreme that they name: `hub_ids`: offsets into the block of features of the same device. `requests`: row d of a device's lists holds offsets into the block of features of the device at shard index d with the same rep index; empty slots hold offsets too. counts[r, s, d] slots of the list from shard index s to shard index d are live, the first ones; for every rep index some destination has 32 live slots from every source. `neighbors`: A code below 256 names a row of the device's hub cache; a code 256 + d * 32 + c names slot c of the device's list to shard index d, and counts only where that slot is live.
All inputs are finite; a program needn't handle non-finite values.
Results may differ from the reference program's by a relative error of at most 0.0003.
Values sent between devices are 32-bit elements; how exact they have to be, the bound alone decides.
A program may use at most 64 MiB of HBM per device.

```python
import jax
import jax.numpy as jnp
from jax import lax

F = 256
FANOUT = 15
CAP = 32
ROWS_DEV = 512
SEEDS_DEV = 128
HUB_DEV = 128
HUBS = 256
SLOTS_DEV = 512
CODES = 768
NODES = 16384
SEEDS = 4096
HUB_SLOTS = 4096
REQ_ROWS = 512
N_REP = 2
N_SHARD = 16


def draw_counts(key, part):
    k_base, k_owner = jax.random.split(jax.random.fold_in(key, 11), 2)
    base_fill = jax.random.randint(k_base, (N_REP, N_SHARD, N_SHARD), CAP // 4, CAP + 1)
    full_owner = jax.random.randint(k_owner, (N_REP, 1, 1), 0, N_SHARD)
    owner_index = lax.broadcasted_iota(jnp.int32, (N_REP, N_SHARD, N_SHARD), 2)
    result = jnp.where(owner_index == full_owner, CAP, base_fill)
    return result.reshape(-1).astype(jnp.int32)


def plant(entries, rng, low, top_value):
    longest = entries.shape.index(max(entries.shape))
    spots = []
    for shift in (0, 1):
        where = [jax.random.randint(jax.random.fold_in(rng, axis), (), 0, length) for axis, length in enumerate(entries.shape)]
        where[longest] = (where[longest] + shift) % entries.shape[longest]
        spots.append(tuple(where))
    return entries.at[spots[0]].set(low).at[spots[1]].set(top_value)


def steps_of(stream_key, extent, shards, low, largest):
    gain = 1.0
    for position, parts in shards:
        steps = jax.random.uniform(jax.random.fold_in(jax.random.fold_in(stream_key, 6), position), (parts,), jnp.float32, low / len(shards), largest / len(shards))
        gain = gain * jnp.repeat(jnp.exp(steps), extent[position] // parts).reshape((-1,) + (1,) * (len(extent) - 1 - position))
    return gain


def bell_draw(rng, extent, deviation, bound, cuts=(), kind=jnp.bfloat16):
    level = steps_of(rng, extent, cuts, -0.22, 0.18) if cuts else 1.0
    values = jax.random.normal(rng, extent, jnp.float32) * deviation * level
    return jnp.minimum(jnp.maximum(values, -bound), bound).astype(kind)


def setup_inputs(seed: int = 0) -> dict:
    seeds = jax.random.split(jax.random.key(seed), 9)
    features = bell_draw(seeds[0], (NODES, F), 1.0, 6.0, ((0, 32),), jnp.float32)
    seed_self = bell_draw(seeds[1], (SEEDS, F), 1.0, 6.0, ((0, 32),), jnp.float32)
    hub_ids = plant(jax.random.randint(seeds[2], (HUB_SLOTS,), 0, ROWS_DEV), jax.random.fold_in(seeds[2], 1), 0, ROWS_DEV - 1).astype(jnp.int32)
    requests = plant(jax.random.randint(seeds[3], (REQ_ROWS, CAP), 0, ROWS_DEV), jax.random.fold_in(seeds[3], 1), 0, ROWS_DEV - 1).astype(jnp.int32)
    counts = draw_counts(jax.random.fold_in(seeds[8], 71), 0)
    neighbors = plant(jax.random.randint(seeds[5], (SEEDS, FANOUT), 0, CODES), jax.random.fold_in(seeds[5], 1), 0, CODES - 1).astype(jnp.int32)
    weight = bell_draw(seeds[6], (F, F), (F // 8) ** -0.5, 1.0, (), jnp.float32)
    out_bias = bell_draw(seeds[7], (F,), 1.0, 4.0, (), jnp.float32)
    return dict(features=features, seed_self=seed_self, hub_ids=hub_ids, requests=requests, counts=counts, neighbors=neighbors, weight=weight, out_bias=out_bias)


def reference(features, seed_self, hub_ids, requests, counts, neighbors, weight, out_bias):
    blocks = features.reshape(N_REP, N_SHARD, ROWS_DEV, F)
    hub_index = hub_ids.reshape(N_REP, N_SHARD, HUB_DEV)
    request_index = requests.reshape(N_REP, N_SHARD, N_SHARD, CAP)
    fill_counts = counts.reshape(N_REP, N_SHARD, N_SHARD)
    neighbor_codes = neighbors.reshape(N_REP * N_SHARD, SEEDS_DEV, FANOUT)
    own_rows = seed_self.reshape(N_REP * N_SHARD, SEEDS_DEV, F)
    rep_iota = jnp.arange(N_REP, dtype=jnp.int32)[:, None]
    shard_iota = jnp.arange(N_SHARD, dtype=jnp.int32)[:, None]
    slot_iota = jnp.arange(CAP, dtype=jnp.int32)[None, :]

    def per_device(device_index):
        rep_pos = device_index // N_SHARD
        shard_pos = device_index % N_SHARD
        hub_cache = blocks[rep_iota, shard_pos, hub_index[:, shard_pos]].reshape(HUBS, F)
        fetched = blocks[rep_pos, shard_iota, request_index[rep_pos, shard_pos]].reshape(SLOTS_DEV, F)
        source = jnp.concatenate([hub_cache, fetched], axis=0)
        slot_live = (slot_iota < fill_counts[rep_pos, shard_pos][:, None]).astype(jnp.float32)
        live = jnp.concatenate([jnp.ones((HUBS,), jnp.float32), slot_live.reshape(SLOTS_DEV)])
        codes = neighbor_codes[device_index]
        picked = source[codes]
        weights = live[codes]
        total = own_rows[device_index] + jnp.sum(picked * weights[:, :, None], axis=1)
        taken = 1.0 + jnp.sum(weights, axis=1)
        mean_rows = total / taken[:, None]
        product = jnp.dot(mean_rows, weight, precision=lax.Precision.HIGHEST, preferred_element_type=jnp.float32)
        return jnp.maximum(product + out_bias, 0.0)

    result = lax.map(per_device, jnp.arange(N_REP * N_SHARD, dtype=jnp.int32))
    return result.reshape(SEEDS, F)
```

```python
import functools

import jax
import jax.numpy as jnp
from jax import lax
from jax.experimental import pallas as pl
from jax.experimental.pallas import tpu as pltpu
from jax.sharding import PartitionSpec as P

LANES = 128


def halves(values):
    high = values.astype(jnp.bfloat16)
    low = (values - high.astype(jnp.float32)).astype(jnp.bfloat16)
    return high, low


def dot(left, right):
    return jnp.dot(left, right, preferred_element_type=jnp.float32)


def columns_of(rows):
    count = rows.shape[0]
    if count < LANES:
        rows = jnp.concatenate([rows, jnp.zeros((LANES - count, LANES), rows.dtype)], axis=0)
    return rows.T


def kernel(
    n, reps, feat_hbm, self_hbm, hub_ref, req_ref, cnt_ref, nbr_ref, weight_hbm, out_ref,
    feat, own, weight, req_send, req_recv, gathered, fetched, hubs,
    local_sem, req_send_sem, req_recv_sem, row_send_sem, row_recv_sem, hub_send_sem, hub_recv_sem,
):
    me = lax.axis_index("shard")
    rep = lax.axis_index("rep")
    rows, width = feat.shape
    cap = req_ref.shape[1]
    hub_dev = hub_ref.shape[1]
    seeds, fanout = nbr_ref.shape
    hub_total = hub_dev * reps

    loads = [
        pltpu.make_async_copy(src, dst, local_sem.at[i])
        for i, (src, dst) in enumerate(((feat_hbm, feat), (weight_hbm, weight), (self_hbm, own)))
    ]
    for load in loads:
        load.start()

    barrier = pltpu.get_barrier_semaphore()
    for off in range(1, n):
        pl.semaphore_signal(barrier, inc=1, device_id={"shard": lax.rem(me + off, n)})
    for off in range(1, reps):
        pl.semaphore_signal(barrier, inc=1, device_id={"rep": lax.rem(rep + off, reps)})

    lists = jnp.concatenate([req_ref[...], jnp.zeros((n, LANES - cap), jnp.int32)], axis=1)
    req_send[...] = lists.reshape(n, 1, LANES)
    req_recv[0] = req_send[me]
    pl.semaphore_wait(barrier, n - 1 + reps - 1)

    asks = []
    for off in range(1, n):
        peer = lax.rem(me + off, n)
        ask = pltpu.make_async_remote_copy(
            src_ref=req_send.at[peer],
            dst_ref=req_recv.at[n - off],
            send_sem=req_send_sem.at[off],
            recv_sem=req_recv_sem.at[n - off],
            device_id={"shard": peer},
        )
        ask.start()
        asks.append(ask)

    loads[0].wait()
    high, low = halves(feat[...])
    row_iota = lax.broadcasted_iota(jnp.int32, (LANES, rows), 1)

    hub_columns = columns_of(jnp.broadcast_to(hub_ref[...], (8, hub_dev)))
    pick = (hub_columns[:, 0:1] == row_iota).astype(jnp.float32).astype(jnp.bfloat16)
    hubs[rep] = dot(pick, high) + dot(pick, low)
    shares = []
    for off in range(1, reps):
        share = pltpu.make_async_remote_copy(
            src_ref=hubs.at[rep],
            dst_ref=hubs.at[rep],
            send_sem=hub_send_sem.at[off],
            recv_sem=hub_recv_sem.at[rep],
            device_id={"rep": lax.rem(rep + off, reps)},
        )
        share.start()
        shares.append(share)

    code_count = hub_total + n * cap
    code_iota = lax.broadcasted_iota(jnp.int32, (seeds, code_count), 1)
    codes = nbr_ref[...]
    tally = jnp.zeros((seeds, code_count), jnp.float32)
    for k in range(fanout):
        tally = tally + (codes[:, k : k + 1] == code_iota).astype(jnp.float32)
    spread = (
        lax.broadcasted_iota(jnp.int32, (n, n * cap), 1) // cap
        == lax.broadcasted_iota(jnp.int32, (n, n * cap), 0)
    ).astype(jnp.float32).astype(jnp.bfloat16)
    fill = jnp.broadcast_to(cnt_ref[...].astype(jnp.float32), (8, n)).astype(jnp.bfloat16)
    slot_fill = dot(fill, spread)[0:1]
    slot_iota = (lax.broadcasted_iota(jnp.int32, (1, n * cap), 1) % cap).astype(jnp.float32)
    slot_live = (slot_iota < slot_fill).astype(jnp.float32)
    hub_tally = tally[:, :hub_total]
    slot_tally = tally[:, hub_total:] * slot_live
    taken = 1.0 + jnp.sum(hub_tally, axis=1, keepdims=True) + jnp.sum(slot_tally, axis=1, keepdims=True)
    scale = 1.0 / taken
    hub_tally = hub_tally.astype(jnp.bfloat16)
    slot_tally = slot_tally.astype(jnp.bfloat16)

    for off in range(1, n):
        asks[off - 1].wait_send()
        pltpu.make_async_copy(req_recv.at[off], req_recv.at[off], req_recv_sem.at[off]).wait()
    request_columns = columns_of(req_recv[...].reshape(n, LANES))
    replies = []
    batch = LANES // cap
    for first in range(0, n, batch):
        pick = jnp.concatenate(
            [
                (request_columns[:cap, off : off + 1] == row_iota[:cap]).astype(jnp.float32)
                for off in range(first, first + batch)
            ],
            axis=0,
        ).astype(jnp.bfloat16)
        gathered[first : first + batch] = (dot(pick, high) + dot(pick, low)).reshape(batch, cap, width)
        for off in range(first, first + batch):
            if off == 0:
                continue
            reply = pltpu.make_async_remote_copy(
                src_ref=gathered.at[off],
                dst_ref=fetched.at[me],
                send_sem=row_send_sem.at[off],
                recv_sem=row_recv_sem.at[me],
                device_id={"shard": lax.rem(me + off, n)},
            )
            reply.start()
            replies.append(reply)
    fetched[me] = gathered[0]

    loads[2].wait()
    for off in range(1, reps):
        shares[off - 1].wait_send()
        other = lax.rem(rep + off, reps)
        pltpu.make_async_copy(hubs.at[other], hubs.at[other], hub_recv_sem.at[other]).wait()
    hub_high, hub_low = halves(hubs[...].reshape(hub_total, width))
    total = own[...] + (dot(hub_tally, hub_high) + dot(hub_tally, hub_low))
    loads[1].wait()
    weight_high, weight_low = halves(weight[...])

    for off in range(1, n):
        owner = lax.rem(me + off, n)
        pltpu.make_async_copy(fetched.at[owner], fetched.at[owner], row_recv_sem.at[owner]).wait()
    row_high, row_low = halves(fetched[...].reshape(n * cap, width))
    total = total + (dot(slot_tally, row_high) + dot(slot_tally, row_low))
    mean_high, mean_low = halves(total * scale)
    out_ref[...] = dot(mean_high, weight_high) + (dot(mean_high, weight_low) + dot(mean_low, weight_high))
    for reply in replies:
        reply.wait_send()


def local(n, reps, features, seed_self, hub_ids, requests, counts, neighbors, weight, out_bias):
    rows, width = features.shape
    cap = requests.shape[1]
    hub_dev = hub_ids.shape[0]
    seeds = neighbors.shape[0]
    hbm = pl.BlockSpec(memory_space=pl.ANY)
    vmem = pl.BlockSpec(memory_space=pltpu.VMEM)
    dma = pltpu.SemaphoreType.DMA
    product = pl.pallas_call(
        functools.partial(kernel, n, reps),
        out_shape=jax.ShapeDtypeStruct((seeds, width), jnp.float32),
        in_specs=[hbm, hbm, vmem, vmem, vmem, vmem, hbm],
        out_specs=vmem,
        scratch_shapes=[
            pltpu.VMEM((rows, width), jnp.float32),
            pltpu.VMEM((seeds, width), jnp.float32),
            pltpu.VMEM(weight.shape, jnp.float32),
            pltpu.VMEM((n, 1, LANES), jnp.int32),
            pltpu.VMEM((n, 1, LANES), jnp.int32),
            pltpu.VMEM((n, cap, width), jnp.float32),
            pltpu.VMEM((n, cap, width), jnp.float32),
            pltpu.VMEM((reps, hub_dev, width), jnp.float32),
            dma((3,)),
            dma((n,)),
            dma((n,)),
            dma((n,)),
            dma((n,)),
            dma((reps,)),
            dma((reps,)),
        ],
        compiler_params=pltpu.CompilerParams(collective_id=0, has_side_effects=True),
    )(features, seed_self, hub_ids[None], requests, counts[None], neighbors, weight)
    return jnp.maximum(product + out_bias, 0.0)


def solution(mesh):
    return jax.shard_map(
        functools.partial(local, mesh.shape["shard"], mesh.shape["rep"]),
        mesh=mesh,
        in_specs=(
            P(("rep", "shard"), None),
            P(("rep", "shard"), None),
            P(("rep", "shard")),
            P(("rep", "shard"), None),
            P(("rep", "shard")),
            P(("rep", "shard"), None),
            P(),
            P(),
        ),
        out_specs=P(("rep", "shard"), None),
        check_vma=False,
    )
```

```python
import functools

import jax
import jax.numpy as jnp
from jax import lax
from jax.experimental import pallas as pl
from jax.experimental.pallas import tpu as pltpu
from jax.sharding import PartitionSpec as P

LANES = 128


def halves(values):
    high = values.astype(jnp.bfloat16)
    low = (values - high.astype(jnp.float32)).astype(jnp.bfloat16)
    return high, low


def dot(left, right):
    return jnp.dot(left, right, preferred_element_type=jnp.float32)


def plan(me, n):
    quarter = n // 4
    block, place = me // quarter, lax.rem(me, quarter)
    side = block // 2
    outer = lax.rem(block + side, 2)
    inner_far = 2 - side
    outer_far = 3 - 3 * side
    sibling = block + 1 - 2 * lax.rem(block, 2)
    blocks = (inner_far, outer_far, sibling, block)
    peers = [[blocks[g] * quarter + lax.rem(place + q, quarter) for q in range(quarter)] for g in range(4)]
    mine = (1 - outer, 1 - outer, 2, 3)
    spots = [[mine[g] * quarter + (quarter - q) % quarter for q in range(quarter)] for g in range(4)]
    return blocks, sum(peers, []), sum(spots, [])


def columns_of(rows):
    count = rows.shape[0]
    if count < LANES:
        rows = jnp.concatenate([rows, jnp.zeros((LANES - count, LANES), rows.dtype)], axis=0)
    return rows.T


def kernel(
    n, reps, feat_hbm, self_hbm, hub_ref, req_ref, cnt_ref, nbr_ref, weight_hbm, out_ref,
    feat, own, weight, req_send, req_recv, gathered, fetched, hubs, slot_tally,
    local_sem, req_send_sem, req_recv_sem, row_send_sem, row_recv_sem, hub_send_sem, hub_recv_sem,
):
    me = lax.axis_index("shard")
    rep = lax.axis_index("rep")
    rows, width = feat.shape
    cap = req_ref.shape[1]
    hub_dev = hub_ref.shape[1]
    fanout, seeds = nbr_ref.shape
    hub_total = hub_dev * reps
    quarter = n // 4
    own_spot = n - quarter
    blocks, peers, spots = plan(me, n)
    others = [i for i in range(n) if i != own_spot]

    loads = [
        pltpu.make_async_copy(src, dst, local_sem.at[i])
        for i, (src, dst) in enumerate(((feat_hbm, feat), (weight_hbm, weight), (self_hbm, own)))
    ]
    for load in loads:
        load.start()

    barrier = pltpu.get_barrier_semaphore()
    for i in others:
        pl.semaphore_signal(barrier, inc=1, device_id={"shard": peers[i]})
    for off in range(1, reps):
        pl.semaphore_signal(barrier, inc=1, device_id={"rep": lax.rem(rep + off, reps)})

    lists = jnp.concatenate([req_ref[...], jnp.zeros((n, LANES - cap), jnp.int32)], axis=1)
    req_send[...] = lists.reshape(n, 1, LANES)
    req_recv[own_spot] = req_send[me]

    loads[0].wait()
    high, low = halves(feat[...])
    row_iota = lax.broadcasted_iota(jnp.int32, (LANES, rows), 1)
    hub_columns = columns_of(jnp.broadcast_to(hub_ref[...], (8, hub_dev)))
    pick = (hub_columns[:, 0:1] == row_iota).astype(jnp.float32).astype(jnp.bfloat16)
    hubs[rep] = dot(pick, high) + dot(pick, low)
    pl.semaphore_wait(barrier, n - 1 + reps - 1)

    asks = []
    for i in others:
        ask = pltpu.make_async_remote_copy(
            src_ref=req_send.at[peers[i]],
            dst_ref=req_recv.at[spots[i]],
            send_sem=req_send_sem.at[i],
            recv_sem=req_recv_sem.at[spots[i]],
            device_id={"shard": peers[i]},
        )
        ask.start()
        asks.append(ask)
    shares = []
    for off in range(1, reps):
        share = pltpu.make_async_remote_copy(
            src_ref=hubs.at[rep],
            dst_ref=hubs.at[rep],
            send_sem=hub_send_sem.at[off],
            recv_sem=hub_recv_sem.at[rep],
            device_id={"rep": lax.rem(rep + off, reps)},
        )
        share.start()
        shares.append(share)

    code_count = hub_total + n * cap
    code_iota = lax.broadcasted_iota(jnp.int32, (seeds, code_count), 1)
    codes = columns_of(nbr_ref[...])
    tally = jnp.zeros((seeds, code_count), jnp.float32)
    for k in range(fanout):
        tally = tally + (codes[:, k : k + 1] == code_iota).astype(jnp.float32)
    spread = (
        lax.broadcasted_iota(jnp.int32, (n, n * cap), 1) // cap
        == lax.broadcasted_iota(jnp.int32, (n, n * cap), 0)
    ).astype(jnp.float32).astype(jnp.bfloat16)
    fill = jnp.broadcast_to(cnt_ref[...].astype(jnp.float32), (8, n)).astype(jnp.bfloat16)
    slot_fill = dot(fill, spread)[0:1]
    slot_iota = (lax.broadcasted_iota(jnp.int32, (1, n * cap), 1) % cap).astype(jnp.float32)
    slot_live = (slot_iota < slot_fill).astype(jnp.float32)
    hub_tally = tally[:, :hub_total]
    live_tally = tally[:, hub_total:] * slot_live
    taken = 1.0 + jnp.sum(hub_tally, axis=1, keepdims=True) + jnp.sum(live_tally, axis=1, keepdims=True)
    scale = 1.0 / taken
    hub_tally = hub_tally.astype(jnp.bfloat16)
    for b in range(4):
        slot_tally[b] = live_tally[:, b * quarter * cap : (b + 1) * quarter * cap].astype(jnp.bfloat16)

    replies = []
    batch = min(LANES // cap, quarter)
    for group in range(4):
        span = range(group * quarter, (group + 1) * quarter)
        for i in span:
            if i != own_spot:
                pltpu.make_async_copy(req_recv.at[i], req_recv.at[i], req_recv_sem.at[i]).wait()
        request_columns = columns_of(req_recv[group * quarter : (group + 1) * quarter].reshape(quarter, LANES))
        for first in range(0, quarter, batch):
            pick = jnp.concatenate(
                [
                    (request_columns[:cap, q : q + 1] == row_iota[:cap]).astype(jnp.float32)
                    for q in range(first, first + batch)
                ],
                axis=0,
            ).astype(jnp.bfloat16)
            base = group * quarter + first
            gathered[base : base + batch] = (dot(pick, high) + dot(pick, low)).reshape(batch, cap, width)
            for i in range(base, base + batch):
                if i == own_spot:
                    continue
                reply = pltpu.make_async_remote_copy(
                    src_ref=gathered.at[i],
                    dst_ref=fetched.at[me],
                    send_sem=row_send_sem.at[i],
                    recv_sem=row_recv_sem.at[me],
                    device_id={"shard": peers[i]},
                )
                reply.start()
                replies.append(reply)
    fetched[me] = gathered[own_spot]
    for ask in asks:
        ask.wait_send()

    loads[2].wait()
    for off in range(1, reps):
        shares[off - 1].wait_send()
        other = lax.rem(rep + off, reps)
        pltpu.make_async_copy(hubs.at[other], hubs.at[other], hub_recv_sem.at[other]).wait()
    hub_high, hub_low = halves(hubs[...].reshape(hub_total, width))
    total = own[...] + (dot(hub_tally, hub_high) + dot(hub_tally, hub_low))
    loads[1].wait()
    weight_high, weight_low = halves(weight[...])

    for group in (3, 2, 0, 1):
        for i in range(group * quarter, (group + 1) * quarter):
            if i != own_spot:
                pltpu.make_async_copy(fetched.at[peers[i]], fetched.at[peers[i]], row_recv_sem.at[peers[i]]).wait()
        block = blocks[group]
        row_high, row_low = halves(fetched[pl.ds(block * quarter, quarter)].reshape(quarter * cap, width))
        counted = slot_tally[block]
        total = total + (dot(counted, row_high) + dot(counted, row_low))
    mean_high, mean_low = halves(total * scale)
    out_ref[...] = dot(mean_high, weight_high) + (dot(mean_high, weight_low) + dot(mean_low, weight_high))
    for reply in replies:
        reply.wait_send()


def local(n, reps, features, seed_self, hub_ids, requests, counts, neighbors, weight, out_bias):
    rows, width = features.shape
    cap = requests.shape[1]
    hub_dev = hub_ids.shape[0]
    seeds = neighbors.shape[0]
    hbm = pl.BlockSpec(memory_space=pltpu.HBM)
    vmem = pl.BlockSpec(memory_space=pltpu.VMEM)
    dma = pltpu.SemaphoreType.DMA
    product = pl.pallas_call(
        functools.partial(kernel, n, reps),
        out_shape=jax.ShapeDtypeStruct((seeds, width), jnp.float32),
        in_specs=[hbm, hbm, vmem, vmem, vmem, vmem, hbm],
        out_specs=vmem,
        scratch_shapes=[
            pltpu.VMEM((rows, width), jnp.float32),
            pltpu.VMEM((seeds, width), jnp.float32),
            pltpu.VMEM(weight.shape, jnp.float32),
            pltpu.VMEM((n, 1, LANES), jnp.int32),
            pltpu.VMEM((n, 1, LANES), jnp.int32),
            pltpu.VMEM((n, cap, width), jnp.float32),
            pltpu.VMEM((n, cap, width), jnp.float32),
            pltpu.VMEM((reps, hub_dev, width), jnp.float32),
            pltpu.VMEM((4, seeds, n // 4 * cap), jnp.bfloat16),
            dma((3,)),
            dma((n,)),
            dma((n,)),
            dma((n,)),
            dma((n,)),
            dma((reps,)),
            dma((reps,)),
        ],
        compiler_params=pltpu.CompilerParams(collective_id=0, has_side_effects=True),
    )(features, seed_self, hub_ids[None], requests, counts[None], neighbors.T, weight)
    return jnp.maximum(product + out_bias, 0.0)


def solution(mesh):
    return jax.shard_map(
        functools.partial(local, mesh.shape["shard"], mesh.shape["rep"]),
        mesh=mesh,
        in_specs=(
            P(("rep", "shard"), None),
            P(("rep", "shard"), None),
            P(("rep", "shard")),
            P(("rep", "shard"), None),
            P(("rep", "shard")),
            P(("rep", "shard"), None),
            P(),
            P(),
        ),
        out_specs=P(("rep", "shard"), None),
        check_vma=False,
    )
```

```python
import functools

import jax
import jax.numpy as jnp
from jax import lax
from jax.experimental import pallas as pl
from jax.experimental.pallas import tpu as pltpu
from jax.sharding import PartitionSpec as P

LANES = 128


def halves(values):
    high = values.astype(jnp.bfloat16)
    low = (values - high.astype(jnp.float32)).astype(jnp.bfloat16)
    return high, low


def dot(left, right):
    return jnp.dot(left, right, preferred_element_type=jnp.float32)


def columns_of(rows):
    count = rows.shape[0]
    if count < LANES:
        rows = jnp.concatenate([rows, jnp.zeros((LANES - count, LANES), rows.dtype)], axis=0)
    return rows.T


def kernel(
    n, reps, feat_hbm, self_hbm, hub_ref, req_ref, cnt_ref, nbr_ref, weight_hbm, out_ref,
    feat, own, weight, table, tables, req_recv, gathered, fetched, hubs, slot_tally,
    local_sem, ask_sem, req_recv_sem, table_send_sem, table_recv_sem, row_send_sem, row_recv_sem, hub_send_sem, hub_recv_sem,
):
    me = lax.axis_index("shard")
    rep = lax.axis_index("rep")
    rows, width = feat.shape
    cap = req_ref.shape[1]
    hub_dev = hub_ref.shape[1]
    fanout, seeds = nbr_ref.shape
    hub_total = hub_dev * reps
    quarter = n // 4
    block, place = me // quarter, lax.rem(me, quarter)
    side = block // 2
    inner = lax.rem(block + side, 2)
    is_inner = inner == 1
    near = 1 + lax.rem(block, 2)
    edge = 3 * side
    twin = 3 - block
    far = 3 - edge
    turns = [lax.rem(place + q, quarter) for q in range(quarter)]

    loads = [
        pltpu.make_async_copy(src, dst, local_sem.at[i])
        for i, (src, dst) in enumerate(((feat_hbm, feat), (weight_hbm, weight), (self_hbm, own)))
    ]
    for load in loads:
        load.start()

    barrier = pltpu.get_barrier_semaphore()

    def greet(peer_block, places):
        for spot in places:
            pl.semaphore_signal(barrier, inc=1, device_id={"shard": peer_block * quarter + spot})

    greet(block, turns[1:])
    greet(near, turns)

    @pl.when(is_inner)
    def _():
        greet(edge, turns)

    for off in range(1, reps):
        pl.semaphore_signal(barrier, inc=1, device_id={"rep": lax.rem(rep + off, reps)})

    lists = jnp.concatenate([req_ref[...], jnp.zeros((n, LANES - cap), jnp.int32)], axis=1)
    table[...] = lists.reshape(4, quarter, 1, LANES)
    req_recv[block, place] = table[block, place]
    pl.semaphore_wait(barrier, quarter - 1 + quarter + quarter * inner + reps - 1)

    def row_copies(source, owner_block, to_block, lane, places):
        return [
            pltpu.make_async_remote_copy(
                src_ref=source.at[to_block, spot],
                dst_ref=req_recv.at[owner_block, place],
                send_sem=ask_sem.at[lane, q],
                recv_sem=req_recv_sem.at[owner_block, place],
                device_id={"shard": to_block * quarter + spot},
            )
            for q, spot in enumerate(places)
        ]

    def table_copy(source, to_block, slot, lane):
        return pltpu.make_async_remote_copy(
            src_ref=source,
            dst_ref=tables.at[slot],
            send_sem=table_send_sem.at[lane],
            recv_sem=table_recv_sem.at[slot],
            device_id={"shard": to_block * quarter + place},
        )

    def start(copies):
        for copy in copies:
            copy.start()

    def sent(copies):
        for copy in copies:
            copy.wait_send()

    def table_wait(slot):
        pltpu.make_async_copy(tables.at[slot], tables.at[slot], table_recv_sem.at[slot]).wait()

    asks = row_copies(table, block, near, 0, turns) + row_copies(table, block, block, 1, turns[1:])
    edge_asks = row_copies(table, block, edge, 2, turns)
    own_table = table_copy(table, near, inner, 0)
    passed = [
        row_copies(tables.at[0], edge, twin, 3, turns) + [table_copy(tables.at[0], twin, 2, 1)],
        row_copies(tables.at[1], twin, edge, 4, turns),
        row_copies(tables.at[2], far, edge, 5, turns),
    ]

    own_table.start()
    start(asks)

    @pl.when(is_inner)
    def _():
        start(edge_asks)

    loads[0].wait()
    high, low = halves(feat[...])
    row_iota = lax.broadcasted_iota(jnp.int32, (LANES, rows), 1)

    @pl.when(is_inner)
    def _():
        for slot in (0, 1):
            table_wait(slot)
            start(passed[slot])

    batch = min(LANES // cap, quarter)

    def reply_copy(group, owner_block, q):
        spot = turns[q]
        return pltpu.make_async_remote_copy(
            src_ref=gathered.at[group, spot],
            dst_ref=fetched.at[me],
            send_sem=row_send_sem.at[group, q],
            recv_sem=row_recv_sem.at[me],
            device_id={"shard": owner_block * quarter + spot},
        )

    def unless_own(peer_block, q, action):
        if q:
            action()
        else:
            pl.when(peer_block != block)(action)

    def answer(group, peer_block):
        for q, spot in enumerate(turns):
            ref = req_recv.at[peer_block, spot]
            unless_own(peer_block, q, pltpu.make_async_copy(ref, ref, req_recv_sem.at[peer_block, spot]).wait)
        request_columns = columns_of(req_recv[peer_block].reshape(quarter, LANES))
        for first in range(0, quarter, batch):
            pick = jnp.concatenate(
                [
                    (request_columns[:cap, q : q + 1] == row_iota[:cap]).astype(jnp.float32)
                    for q in range(first, first + batch)
                ],
                axis=0,
            ).astype(jnp.bfloat16)
            picked = dot(pick, high) + dot(pick, low)
            gathered[group, first : first + batch] = picked.reshape(batch, cap, width)
        for q in range(quarter):
            unless_own(peer_block, q, reply_copy(group, peer_block, q).start)

    peer_blocks = (near, edge, 2 - lax.rem(block, 2), far)
    own_group = 1 + inner
    for group in range(3):
        answer(group, peer_blocks[group])

    @pl.when(is_inner)
    def _():
        table_wait(2)
        start(passed[2])

    answer(3, peer_blocks[3])
    fetched[me] = gathered[own_group, place]

    hub_columns = columns_of(jnp.broadcast_to(hub_ref[...], (8, hub_dev)))
    pick = (hub_columns[:, 0:1] == row_iota).astype(jnp.float32).astype(jnp.bfloat16)
    hubs[rep] = dot(pick, high) + dot(pick, low)
    shares = []
    for off in range(1, reps):
        share = pltpu.make_async_remote_copy(
            src_ref=hubs.at[rep],
            dst_ref=hubs.at[rep],
            send_sem=hub_send_sem.at[off],
            recv_sem=hub_recv_sem.at[rep],
            device_id={"rep": lax.rem(rep + off, reps)},
        )
        share.start()
        shares.append(share)

    code_count = hub_total + n * cap
    code_iota = lax.broadcasted_iota(jnp.int32, (seeds, code_count), 1)
    codes = columns_of(nbr_ref[...])
    tally = jnp.zeros((seeds, code_count), jnp.float32)
    for k in range(fanout):
        tally = tally + (codes[:, k : k + 1] == code_iota).astype(jnp.float32)
    spread = (
        lax.broadcasted_iota(jnp.int32, (n, n * cap), 1) // cap
        == lax.broadcasted_iota(jnp.int32, (n, n * cap), 0)
    ).astype(jnp.float32).astype(jnp.bfloat16)
    fill = jnp.broadcast_to(cnt_ref[...].astype(jnp.float32), (8, n)).astype(jnp.bfloat16)
    slot_fill = dot(fill, spread)[0:1]
    slot_iota = (lax.broadcasted_iota(jnp.int32, (1, n * cap), 1) % cap).astype(jnp.float32)
    slot_live = (slot_iota < slot_fill).astype(jnp.float32)
    hub_tally = tally[:, :hub_total]
    live_tally = tally[:, hub_total:] * slot_live
    taken = 1.0 + jnp.sum(hub_tally, axis=1, keepdims=True) + jnp.sum(live_tally, axis=1, keepdims=True)
    scale = 1.0 / taken
    hub_tally = hub_tally.astype(jnp.bfloat16)
    for b in range(4):
        slot_tally[b] = live_tally[:, b * quarter * cap : (b + 1) * quarter * cap].astype(jnp.bfloat16)

    own_table.wait_send()
    sent(asks)

    @pl.when(is_inner)
    def _():
        sent(edge_asks)
        for copies in passed:
            sent(copies)

    loads[2].wait()
    for off in range(1, reps):
        shares[off - 1].wait_send()
        other = lax.rem(rep + off, reps)
        pltpu.make_async_copy(hubs.at[other], hubs.at[other], hub_recv_sem.at[other]).wait()
    hub_high, hub_low = halves(hubs[...].reshape(hub_total, width))
    total = own[...] + (dot(hub_tally, hub_high) + dot(hub_tally, hub_low))
    loads[1].wait()
    weight_high, weight_low = halves(weight[...])

    for owner_block in (block, block + 1 - 2 * lax.rem(block, 2), 2 - side, far):
        for q, spot in enumerate(turns):
            ref = fetched.at[owner_block * quarter + spot]
            unless_own(owner_block, q, pltpu.make_async_copy(ref, ref, row_recv_sem.at[owner_block * quarter + spot]).wait)
        row_high, row_low = halves(fetched[pl.ds(owner_block * quarter, quarter)].reshape(quarter * cap, width))
        counted = slot_tally[owner_block]
        total = total + (dot(counted, row_high) + dot(counted, row_low))
    mean_high, mean_low = halves(total * scale)
    out_ref[...] = dot(mean_high, weight_high) + (dot(mean_high, weight_low) + dot(mean_low, weight_high))
    for group in range(4):
        for q in range(quarter):
            unless_own(peer_blocks[group], q, reply_copy(group, peer_blocks[group], q).wait_send)


def local(n, reps, features, seed_self, hub_ids, requests, counts, neighbors, weight, out_bias):
    rows, width = features.shape
    cap = requests.shape[1]
    hub_dev = hub_ids.shape[0]
    seeds = neighbors.shape[0]
    hbm = pl.BlockSpec(memory_space=pltpu.HBM)
    vmem = pl.BlockSpec(memory_space=pltpu.VMEM)
    dma = pltpu.SemaphoreType.DMA
    product = pl.pallas_call(
        functools.partial(kernel, n, reps),
        out_shape=jax.ShapeDtypeStruct((seeds, width), jnp.float32),
        in_specs=[hbm, hbm, vmem, vmem, vmem, vmem, hbm],
        out_specs=vmem,
        scratch_shapes=[
            pltpu.VMEM((rows, width), jnp.float32),
            pltpu.VMEM((seeds, width), jnp.float32),
            pltpu.VMEM(weight.shape, jnp.float32),
            pltpu.VMEM((4, n // 4, 1, LANES), jnp.int32),
            pltpu.VMEM((3, 4, n // 4, 1, LANES), jnp.int32),
            pltpu.VMEM((4, n // 4, 1, LANES), jnp.int32),
            pltpu.VMEM((4, n // 4, cap, width), jnp.float32),
            pltpu.VMEM((n, cap, width), jnp.float32),
            pltpu.VMEM((reps, hub_dev, width), jnp.float32),
            pltpu.VMEM((4, seeds, n // 4 * cap), jnp.bfloat16),
            dma((3,)),
            dma((6, n // 4)),
            dma((4, n // 4)),
            dma((2,)),
            dma((3,)),
            dma((4, n // 4)),
            dma((n,)),
            dma((reps,)),
            dma((reps,)),
        ],
        compiler_params=pltpu.CompilerParams(collective_id=0, has_side_effects=True),
    )(features, seed_self, hub_ids[None], requests, counts[None], neighbors.T, weight)
    return jnp.maximum(product + out_bias, 0.0)


def solution(mesh):
    return jax.shard_map(
        functools.partial(local, mesh.shape["shard"], mesh.shape["rep"]),
        mesh=mesh,
        in_specs=(
            P(("rep", "shard"), None),
            P(("rep", "shard"), None),
            P(("rep", "shard")),
            P(("rep", "shard"), None),
            P(("rep", "shard")),
            P(("rep", "shard"), None),
            P(),
            P(),
        ),
        out_specs=P(("rep", "shard"), None),
        check_vma=False,
    )
```

```python
import functools

import jax
import jax.numpy as jnp
from jax import lax
from jax.experimental import pallas as pl
from jax.experimental.pallas import tpu as pltpu
from jax.sharding import PartitionSpec as P

LANES = 128


def halves(values):
    high = values.astype(jnp.bfloat16)
    low = (values - high.astype(jnp.float32)).astype(jnp.bfloat16)
    return high, low


def dot(left, right):
    return jnp.dot(left, right, preferred_element_type=jnp.float32)


def columns_of(rows):
    count = rows.shape[0]
    if count < LANES:
        rows = jnp.concatenate([rows, jnp.zeros((LANES - count, LANES), rows.dtype)], axis=0)
    return rows.T


def kernel(
    n, reps, feat_hbm, self_hbm, hub_ref, req_ref, cnt_ref, nbr_ref, weight_hbm, out_ref,
    feat, own, weight, table, tables, req_recv, gathered, fetched, hubs, slot_tally,
    local_sem, ask_sem, req_recv_sem, table_send_sem, table_recv_sem, row_send_sem, row_recv_sem, hub_send_sem, hub_recv_sem,
):
    me = lax.axis_index("shard")
    rep = lax.axis_index("rep")
    rows, width = feat.shape
    cap = req_ref.shape[1]
    hub_dev = hub_ref.shape[1]
    fanout, seeds = nbr_ref.shape
    hub_total = hub_dev * reps
    quarter = n // 4
    block, place = me // quarter, lax.rem(me, quarter)
    side = block // 2
    inner = lax.rem(block + side, 2)
    is_inner = inner == 1
    near = 1 + lax.rem(block, 2)
    edge = 3 * side
    twin = 3 - block
    far = 3 - edge
    turns = [lax.rem(place + q, quarter) for q in range(quarter)]

    loads = [
        pltpu.make_async_copy(src, dst, local_sem.at[i])
        for i, (src, dst) in enumerate(((feat_hbm, feat), (weight_hbm, weight), (self_hbm, own)))
    ]
    for load in loads:
        load.start()

    barrier = pltpu.get_barrier_semaphore()

    def greet(peer_block, places):
        for spot in places:
            pl.semaphore_signal(barrier, inc=1, device_id={"shard": peer_block * quarter + spot})

    greet(block, turns[1:])
    greet(near, turns)

    @pl.when(is_inner)
    def _():
        greet(edge, turns)

    for off in range(1, reps):
        pl.semaphore_signal(barrier, inc=1, device_id={"rep": lax.rem(rep + off, reps)})

    lists = jnp.concatenate([req_ref[...], jnp.zeros((n, LANES - cap), jnp.int32)], axis=1)
    table[...] = lists.reshape(4, quarter, 1, LANES)
    req_recv[block, place] = table[block, place]
    pl.semaphore_wait(barrier, quarter - 1 + quarter + quarter * inner + reps - 1)

    def row_copies(source, owner_block, to_block, lane, places):
        return [
            pltpu.make_async_remote_copy(
                src_ref=source.at[to_block, spot],
                dst_ref=req_recv.at[owner_block, place],
                send_sem=ask_sem.at[lane, q],
                recv_sem=req_recv_sem.at[owner_block, place],
                device_id={"shard": to_block * quarter + spot},
            )
            for q, spot in enumerate(places)
        ]

    def table_copy(source, to_block, slot, lane):
        return pltpu.make_async_remote_copy(
            src_ref=source,
            dst_ref=tables.at[slot],
            send_sem=table_send_sem.at[lane],
            recv_sem=table_recv_sem.at[slot],
            device_id={"shard": to_block * quarter + place},
        )

    def start(copies):
        for copy in copies:
            copy.start()

    def sent(copies):
        for copy in copies:
            copy.wait_send()

    def table_wait(slot):
        pltpu.make_async_copy(tables.at[slot], tables.at[slot], table_recv_sem.at[slot]).wait()

    asks = row_copies(table, block, near, 0, turns) + row_copies(table, block, block, 1, turns[1:])
    edge_asks = row_copies(table, block, edge, 2, turns)
    own_table = table_copy(table, near, inner, 0)
    passed = [
        row_copies(tables.at[0], edge, twin, 3, turns) + [table_copy(tables.at[0], twin, 2, 1)],
        row_copies(tables.at[1], twin, edge, 4, turns),
        row_copies(tables.at[2], far, edge, 5, turns),
    ]

    own_table.start()
    start(asks)

    @pl.when(is_inner)
    def _():
        start(edge_asks)

    loads[0].wait()
    high, low = halves(feat[...])
    row_iota = lax.broadcasted_iota(jnp.int32, (LANES, rows), 1)

    @pl.when(is_inner)
    def _():
        for slot in (0, 1):
            table_wait(slot)
            start(passed[slot])

    batch = min(LANES // cap, quarter)

    def reply_copy(group, owner_block, q):
        spot = turns[q]
        return pltpu.make_async_remote_copy(
            src_ref=gathered.at[group, spot],
            dst_ref=fetched.at[me],
            send_sem=row_send_sem.at[group, q],
            recv_sem=row_recv_sem.at[me],
            device_id={"shard": owner_block * quarter + spot},
        )

    def unless_own(peer_block, q, action):
        if q:
            action()
        else:
            pl.when(peer_block != block)(action)

    def answer(group, peer_block):
        for q, spot in enumerate(turns):
            ref = req_recv.at[peer_block, spot]
            unless_own(peer_block, q, pltpu.make_async_copy(ref, ref, req_recv_sem.at[peer_block, spot]).wait)
        request_columns = columns_of(req_recv[peer_block].reshape(quarter, LANES))
        for first in range(0, quarter, batch):
            pick = jnp.concatenate(
                [
                    (request_columns[:cap, q : q + 1] == row_iota[:cap]).astype(jnp.float32)
                    for q in range(first, first + batch)
                ],
                axis=0,
            ).astype(jnp.bfloat16)
            picked = dot(pick, high) + dot(pick, low)
            gathered[group, first : first + batch] = picked.reshape(batch, cap, width)
        for q in range(quarter):
            unless_own(peer_block, q, reply_copy(group, peer_block, q).start)

    apart = 2 - lax.rem(block, 2)
    peer_blocks = (near, inner * edge + (1 - inner) * apart, far, block)
    own_group = 3
    for group in range(2):
        answer(group, peer_blocks[group])

    @pl.when(is_inner)
    def _():
        table_wait(2)
        start(passed[2])

    for group in range(2, 4):
        answer(group, peer_blocks[group])
    fetched[me] = gathered[own_group, place]

    hub_columns = columns_of(jnp.broadcast_to(hub_ref[...], (8, hub_dev)))
    pick = (hub_columns[:, 0:1] == row_iota).astype(jnp.float32).astype(jnp.bfloat16)
    hubs[rep] = dot(pick, high) + dot(pick, low)
    shares = []
    for off in range(1, reps):
        share = pltpu.make_async_remote_copy(
            src_ref=hubs.at[rep],
            dst_ref=hubs.at[rep],
            send_sem=hub_send_sem.at[off],
            recv_sem=hub_recv_sem.at[rep],
            device_id={"rep": lax.rem(rep + off, reps)},
        )
        share.start()
        shares.append(share)

    code_count = hub_total + n * cap
    code_iota = lax.broadcasted_iota(jnp.int32, (seeds, code_count), 1)
    codes = columns_of(nbr_ref[...])
    tally = jnp.zeros((seeds, code_count), jnp.float32)
    for k in range(fanout):
        tally = tally + (codes[:, k : k + 1] == code_iota).astype(jnp.float32)
    spread = (
        lax.broadcasted_iota(jnp.int32, (n, n * cap), 1) // cap
        == lax.broadcasted_iota(jnp.int32, (n, n * cap), 0)
    ).astype(jnp.float32).astype(jnp.bfloat16)
    fill = jnp.broadcast_to(cnt_ref[...].astype(jnp.float32), (8, n)).astype(jnp.bfloat16)
    slot_fill = dot(fill, spread)[0:1]
    slot_iota = (lax.broadcasted_iota(jnp.int32, (1, n * cap), 1) % cap).astype(jnp.float32)
    slot_live = (slot_iota < slot_fill).astype(jnp.float32)
    hub_tally = tally[:, :hub_total]
    live_tally = tally[:, hub_total:] * slot_live
    taken = 1.0 + jnp.sum(hub_tally, axis=1, keepdims=True) + jnp.sum(live_tally, axis=1, keepdims=True)
    scale = 1.0 / taken
    hub_tally = hub_tally.astype(jnp.bfloat16)
    for b in range(4):
        slot_tally[b] = live_tally[:, b * quarter * cap : (b + 1) * quarter * cap].astype(jnp.bfloat16)

    own_table.wait_send()
    sent(asks)

    @pl.when(is_inner)
    def _():
        sent(edge_asks)
        for copies in passed:
            sent(copies)

    loads[2].wait()
    for off in range(1, reps):
        shares[off - 1].wait_send()
        other = lax.rem(rep + off, reps)
        pltpu.make_async_copy(hubs.at[other], hubs.at[other], hub_recv_sem.at[other]).wait()
    hub_high, hub_low = halves(hubs[...].reshape(hub_total, width))
    total = own[...] + (dot(hub_tally, hub_high) + dot(hub_tally, hub_low))
    loads[1].wait()
    weight_high, weight_low = halves(weight[...])

    for owner_block in (block, block + 1 - 2 * lax.rem(block, 2), 2 - side, far):
        for q, spot in enumerate(turns):
            ref = fetched.at[owner_block * quarter + spot]
            unless_own(owner_block, q, pltpu.make_async_copy(ref, ref, row_recv_sem.at[owner_block * quarter + spot]).wait)
        row_high, row_low = halves(fetched[pl.ds(owner_block * quarter, quarter)].reshape(quarter * cap, width))
        counted = slot_tally[owner_block]
        total = total + (dot(counted, row_high) + dot(counted, row_low))
    mean_high, mean_low = halves(total * scale)
    out_ref[...] = dot(mean_high, weight_high) + (dot(mean_high, weight_low) + dot(mean_low, weight_high))
    for group in range(4):
        for q in range(quarter):
            unless_own(peer_blocks[group], q, reply_copy(group, peer_blocks[group], q).wait_send)


def local(n, reps, features, seed_self, hub_ids, requests, counts, neighbors, weight, out_bias):
    rows, width = features.shape
    cap = requests.shape[1]
    hub_dev = hub_ids.shape[0]
    seeds = neighbors.shape[0]
    hbm = pl.BlockSpec(memory_space=pltpu.HBM)
    vmem = pl.BlockSpec(memory_space=pltpu.VMEM)
    dma = pltpu.SemaphoreType.DMA
    product = pl.pallas_call(
        functools.partial(kernel, n, reps),
        out_shape=jax.ShapeDtypeStruct((seeds, width), jnp.float32),
        in_specs=[hbm, hbm, vmem, vmem, vmem, vmem, hbm],
        out_specs=vmem,
        scratch_shapes=[
            pltpu.VMEM((rows, width), jnp.float32),
            pltpu.VMEM((seeds, width), jnp.float32),
            pltpu.VMEM(weight.shape, jnp.float32),
            pltpu.VMEM((4, n // 4, 1, LANES), jnp.int32),
            pltpu.VMEM((3, 4, n // 4, 1, LANES), jnp.int32),
            pltpu.VMEM((4, n // 4, 1, LANES), jnp.int32),
            pltpu.VMEM((4, n // 4, cap, width), jnp.float32),
            pltpu.VMEM((n, cap, width), jnp.float32),
            pltpu.VMEM((reps, hub_dev, width), jnp.float32),
            pltpu.VMEM((4, seeds, n // 4 * cap), jnp.bfloat16),
            dma((3,)),
            dma((6, n // 4)),
            dma((4, n // 4)),
            dma((2,)),
            dma((3,)),
            dma((4, n // 4)),
            dma((n,)),
            dma((reps,)),
            dma((reps,)),
        ],
        compiler_params=pltpu.CompilerParams(collective_id=0, has_side_effects=True),
    )(features, seed_self, hub_ids[None], requests, counts[None], neighbors.T, weight)
    return jnp.maximum(product + out_bias, 0.0)


def solution(mesh):
    return jax.shard_map(
        functools.partial(local, mesh.shape["shard"], mesh.shape["rep"]),
        mesh=mesh,
        in_specs=(
            P(("rep", "shard"), None),
            P(("rep", "shard"), None),
            P(("rep", "shard")),
            P(("rep", "shard"), None),
            P(("rep", "shard")),
            P(("rep", "shard"), None),
            P(),
            P(),
        ),
        out_specs=P(("rep", "shard"), None),
        check_vma=False,
    )
```
